32 devices in a mesh: gx: 4 (over y, x), gy: 4 (over z), gz: 2 (over core).
Axes of the slice: x: 2, y: 2, z: 4, core: 2. Of those that a mesh axis runs over, the one named last changes fastest.
Arguments:
- start: float32 [4, 4, 2, 1, 32, 1024], P('gx', 'gy', 'gz'), may hold values from -6 to 6
- stencils: float32 [6, 4, 4, 2, 32, 32], P(None, 'gx', 'gy', 'gz'), as said below
Outputs:
- basis: float32 [4, 4, 2, 1, 5, 32, 1024], P('gx', 'gy', 'gz')
- coefficients: float32 [1, 2, 5], replicated
The draws below stay inside these ranges and needn't reach their ends.
Inputs may be any that keep to these rules, and one draw needn't show every extreme that they name: `stencils`: each of a patch's six matrices is symmetric positive definite.
All inputs are finite; a program needn't handle non-finite values.
Results may differ from the reference program's by a relative error of at most 0.0003.
Values sent between devices are 32-bit elements; how exact they have to be, the bound alone decides.
A program may use at most 128 MiB of HBM per device.

```python
import jax
import jax.numpy as jnp
from jax import lax

C = 32
PROBES = 1
ITERS = 5
PATCH_X = 4
PATCH_Y = 4
PATCH_Z = 2
N_GX = 4
N_GY = 4
N_GZ = 2


def draw_stencils(key, part):
    key_entries = jax.random.fold_in(key, 11)
    key_scale = jax.random.fold_in(key, 12)
    shape = (6, PATCH_X, PATCH_Y, PATCH_Z, C, C)
    entries = jax.random.normal(key_entries, shape, jnp.float32)
    rows = jnp.arange(C)
    band = (jnp.abs(rows[:, None] - rows[None, :]) <= 4).astype(jnp.float32)
    factor = entries * band
    square = jnp.einsum('...ij,...kj->...ik', factor, factor) / 9.0
    square = square + 0.5 * jnp.eye(C, dtype=jnp.float32)
    scales = jnp.exp(jax.random.uniform(key_scale, (6, PATCH_X, PATCH_Y, PATCH_Z, 1, 1), jnp.float32, -0.7, 0.7))
    return (square * scales).astype(jnp.float32)


def level_of(stream_key, shape, cuts, smallest, high):
    loudness = 1.0
    for axis_at, blocks in cuts:
        steps = jax.random.uniform(jax.random.fold_in(jax.random.fold_in(stream_key, 6), axis_at), (blocks,), jnp.float32, smallest / len(cuts), high / len(cuts))
        loudness = loudness * jnp.repeat(jnp.exp(steps), shape[axis_at] // blocks).reshape((-1,) + (1,) * (len(shape) - 1 - axis_at))
    return loudness


def bell_draw(rng, extent, spread, bound, pieces=(), held_as=jnp.bfloat16):
    result = jax.random.normal(rng, extent, jnp.float32) * spread
    if len(pieces) > 0:
        result = level_of(rng, extent, pieces, -0.22, 0.18) * result
    return jnp.clip(result, min=-bound, max=bound).astype(held_as)


def setup_inputs(seed: int = 0) -> dict:
    splits = jax.random.split(jax.random.key(seed), 3)
    return {
        "start": bell_draw(splits[0], (PATCH_X, PATCH_Y, PATCH_Z, PROBES, C, C * C), 1.0, 6.0, ((0, 4), (1, 4), (2, 2)), jnp.float32),
        "stencils": draw_stencils(jax.random.fold_in(splits[2], 71), 0),
    }


def along(field, stencils, which, dim):
    grid = field.reshape(N_GX, C, N_GY, C, N_GZ, C)
    matrix = stencils[which]
    forms = ['xaybzc,xyzea->xeybzc', 'xaybzc,xyzeb->xayezc', 'xaybzc,xyzec->xaybze']
    out = jnp.einsum(forms[dim], grid, matrix, precision=lax.Precision.HIGHEST)
    return out.reshape(N_GX * C, N_GY * C, N_GZ * C)

def fold(field, dim, groups):
    moved = jnp.moveaxis(field, dim, 0)
    rest = moved.shape[1:]
    blocks = moved.reshape((groups, C) + rest)
    zero_row = jnp.zeros((1,) + rest, jnp.float32)
    first = blocks[:, 0] + jnp.concatenate([zero_row, blocks[:-1, C - 1]], axis=0)
    last = blocks[:, C - 1] + jnp.concatenate([blocks[1:, 0], zero_row], axis=0)
    blocks = blocks.at[:, 0].set(first).at[:, C - 1].set(last)
    return jnp.moveaxis(blocks.reshape((groups * C,) + rest), 0, dim)

def assemble(field):
    field = fold(field, 0, N_GX)
    field = fold(field, 1, N_GY)
    return fold(field, 2, N_GZ)

def weight_vector(groups):
    index = jnp.arange(groups * C)
    plane = index % C
    block = index // C
    shared = (plane == 0) & (block > 0) | (plane == C - 1) & (block < groups - 1)
    return jnp.where(shared, 0.5, 1.0).astype(jnp.float32)

def operate(field, stencils):
    first = along(field, stencils, 5, 2)
    second = along(first, stencils, 4, 1)
    term_one = along(second, stencils, 0, 0)
    third = along(first, stencils, 1, 1)
    fourth = along(field, stencils, 2, 2)
    fifth = along(fourth, stencils, 4, 1)
    term_two = along(third + fifth, stencils, 3, 0)
    return assemble(term_one + term_two)

def single(start_one, stencils, weights):
    first = assemble(weights * start_one)
    vector = first / jnp.sqrt(jnp.sum(weights * first * first))
    vectors = [vector]
    alphas = []
    betas = []
    for j in range(ITERS):
        image = operate(vectors[j], stencils)
        alpha = jnp.sum(weights * image * vectors[j])
        image = image - alpha * vectors[j]
        if j > 0:
            image = image - betas[j - 1] * vectors[j - 1]
        heights = [jnp.sum(weights * basis_vec * image) for basis_vec in vectors]
        for i in range(j + 1):
            image = image - heights[i] * vectors[i]
        beta = jnp.sqrt(jnp.sum(weights * image * image))
        vectors.append(image / beta)
        alphas.append(alpha)
        betas.append(beta)
    coeffs = jnp.stack([jnp.stack(alphas), jnp.stack(betas)])
    return (jnp.stack(vectors[1:]), coeffs)

def reference(start, stencils):
    weights = weight_vector(N_GX)[:, None, None] * weight_vector(N_GY)[None, :, None] * weight_vector(N_GZ)[None, None, :]
    seven = start.reshape(N_GX, N_GY, N_GZ, PROBES, C, C, C)
    whole = jnp.transpose(seven, (3, 0, 4, 1, 5, 2, 6)).reshape(PROBES, N_GX * C, N_GY * C, N_GZ * C)
    basis_whole, coefficients = lax.map(lambda one: single(one, stencils, weights), whole)
    split = basis_whole.reshape(PROBES, ITERS, N_GX, C, N_GY, C, N_GZ, C)
    basis = jnp.transpose(split, (2, 4, 6, 0, 1, 3, 5, 7)).reshape(N_GX, N_GY, N_GZ, PROBES, ITERS, C, C * C)
    return (basis, coefficients)
```

```python
import functools

import jax
import jax.numpy as jnp
from jax import lax
from jax.experimental import pallas as pl
from jax.experimental.pallas import tpu as pltpu
from jax.sharding import PartitionSpec as P

ITERS = 5
LANES = 128
SUB = 8
MESH = pl.DeviceIdType.MESH
F32 = jnp.float32
BF16 = jnp.bfloat16
HIGHEST = lax.Precision.HIGHEST


def iota(shape, dim):
    return lax.broadcasted_iota(jnp.int32, shape, dim)


def split(x):
    hi = x.astype(BF16)
    return hi, (x - hi.astype(F32)).astype(BF16)


def exact(a, b):
    return lax.dot_general(a, b, (((1,), (0,)), ((), ())), precision=HIGHEST, preferred_element_type=F32)


def mul(a, b):
    return jnp.dot(a, b, preferred_element_type=F32)


def swap(x):
    sub = iota((1, SUB, LANES), 1)
    group = iota((1, SUB, LANES), 2) >> 5
    s0, s1 = sub & 1, (sub >> 1) & 1
    g0, g1 = group & 1, (group >> 1) & 1
    far = pltpu.roll(x, 64, 2)
    x = jnp.where(s1 == g1, x, jnp.where(s1 == 0, pltpu.roll(far, SUB - 2, 1), pltpu.roll(far, 2, 1)))
    up = pltpu.roll(pltpu.roll(x, SUB - 1, 1), 32, 2)
    down = pltpu.roll(pltpu.roll(x, 1, 1), LANES - 32, 2)
    return jnp.where(s0 == g0, x, jnp.where(s0 == 0, up, down))


def build_matrices(st, mx, my, mz):
    count = st.shape[1]
    wide = LANES
    spread = ((iota((wide, count), 0) & (count - 1)) == iota((wide, count), 1)).astype(F32)
    spread_t = ((iota((count, wide), 1) & (count - 1)) == iota((count, wide), 0)).astype(F32)
    same = (iota((wide, wide), 0) >> 5) == (iota((wide, wide), 1) >> 5)
    for slot, which in ((0, 5), (1, 2)):
        big = exact(exact(spread, st[which].T), spread_t)
        hi, lo = split(jnp.where(same, big, 0.0))
        mz[0:wide, slot * wide:(slot + 1) * wide] = hi
        mz[wide:2 * wide, slot * wide:(slot + 1) * wide] = hi
        mz[2 * wide:3 * wide, slot * wide:(slot + 1) * wide] = lo
    rows = 2 * count
    r = iota((rows, count), 0)
    pick = (((r >> 3) * 4 + (r & 3)) == iota((rows, count), 1)).astype(F32)
    cols = 3 * rows
    l = iota((count, cols), 1) & (rows - 1)
    pick_t = (((l >> 3) * 4 + (l & 3)) == iota((count, cols), 0)).astype(F32)
    same = ((iota((rows, cols), 0) >> 2) & 1) == ((iota((rows, cols), 1) >> 2) & 1)
    middle = (iota((rows, cols), 1) >= rows) & (iota((rows, cols), 1) < 2 * rows)
    for slot, which in ((0, 4), (1, 1)):
        big = jnp.where(same, exact(exact(pick, st[which]), pick_t), 0.0)
        hi = big.astype(BF16).astype(F32)
        my[slot * rows:(slot + 1) * rows, :] = jnp.where(middle, big - hi, hi).astype(BF16)
    cols = 6 * count
    tile = ((iota((count, cols), 1) & (count - 1)) == iota((count, cols), 0)).astype(F32)
    stiff = exact(st[0], tile)
    mass = exact(st[3], tile)
    block = iota((count, cols), 1) >> 5
    big = jnp.where(block < 3, stiff, mass)
    hi = big.astype(BF16).astype(F32)
    mx[...] = jnp.where((block == 1) | (block == 4), big - hi, hi).astype(BF16)


def apply_patch(u, mx, my, mz):
    count, area = u.shape
    ni, nt = count // SUB, area // LANES
    tiles = jnp.concatenate(
        [u[SUB * i:SUB * (i + 1), LANES * t:LANES * (t + 1)] for i in range(ni) for t in range(nt)], axis=0
    )
    tiles = swap(tiles.reshape(ni * nt, SUB, LANES)).reshape(ni * nt * SUB, LANES)
    hi, lo = split(tiles)
    z = mul(jnp.concatenate([hi, lo, hi], axis=1), mz)
    rows = nt * SUB
    packed = []
    for slot in range(2):
        part = z[:, slot * LANES:(slot + 1) * LANES]
        wide = jnp.concatenate([part[rows * i:rows * (i + 1)] for i in range(ni)], axis=1)
        hi, lo = split(wide)
        packed.append(jnp.concatenate([hi, hi, lo], axis=0))
    both = mul(my, packed[0])
    first = both[:rows]
    second = both[rows:] + mul(my[:rows], packed[1])
    pieces = []
    for term in (first, second):
        stacked = jnp.concatenate([term[:, LANES * i:LANES * (i + 1)] for i in range(ni)], axis=0)
        stacked = swap(stacked.reshape(ni * nt, SUB, LANES))
        back = jnp.concatenate(
            [jnp.concatenate([stacked[i * nt + t] for i in range(ni)], axis=0) for t in range(nt)], axis=1
        )
        hi, lo = split(back)
        pieces += [hi, hi, lo]
    return mul(mx, jnp.concatenate(pieces, axis=0))


def kernel(sizes, start, st, basis, coef, mx, my, mz, wt, v0, field,
           zs, zr, xs, xr, ys, yr, es, er, rows, hsend, hrecv, rsend, rrecv):
    nx, ny, nz = sizes
    total = nx * ny * nz
    count, area = start.shape
    nt = area // LANES
    ni = count // SUB
    last = count - 1
    px, py, pz = lax.axis_index("gx"), lax.axis_index("gy"), lax.axis_index("gz")
    me = (px * ny + py) * nz + pz
    coords = (px, py, pz)
    there = [[coords[d] > 0, coords[d] < sizes[d] - 1] for d in range(3)]

    for ref in (zr, xr, yr, er):
        ref[...] = jnp.zeros_like(ref)
    barrier = pltpu.get_barrier_semaphore()

    def peer(k):
        p = lax.rem(me + k, total)
        return (p // (ny * nz), (p // nz) % ny, p % nz)

    def greet(k, carry):
        pl.semaphore_signal(barrier, inc=1, device_id=peer(k), device_id_type=MESH)
        return carry

    lax.fori_loop(1, total, greet, 0)

    def shared(index, d):
        return ((index == 0) & there[d][0]) | ((index == last) & there[d][1])

    lane = iota((count, area), 1)
    ia, ib, ic = iota((count, area), 0), lane >> 5, lane & (count - 1)
    half = lambda index, d: jnp.where(shared(index, d), 0.5, 1.0)
    weight = half(ia, 0) * half(ib, 1) * half(ic, 2)
    wt[...] = weight.astype(F32)
    field[...] = start[...] * wt[...]

    lane_c = iota((count, LANES), 1)
    face_c = (lane_c & (count - 1) == 0) | (lane_c & (count - 1) == last)
    even = (lane_c & 1) == 0
    lane8 = iota((SUB, LANES), 1)
    low8, high8 = lane8 < count, lane8 >= LANES - count
    lane1 = iota((1, LANES), 1)
    diag = iota((SUB, LANES), 0) == lane8

    def tile(t):
        return slice(t * LANES, (t + 1) * LANES)

    def remote(src, dst, phase, slot, target):
        return pltpu.make_async_remote_copy(
            src_ref=src, dst_ref=dst, send_sem=hsend.at[phase, slot], recv_sem=hrecv.at[phase, slot],
            device_id=target, device_id_type=MESH)

    def moved(dx, dy, dz):
        step = lambda d: 0 if d is None else 2 * d - 1
        return (px + step(dx), py + step(dy), pz + step(dz))

    def z_copies(phase):
        return [(remote(zs.at[phase], zr.at[phase, 1 - d], phase, 1 - d, moved(None, None, d)),
                 there[2][d]) for d in range(2)]

    def xy_copies(phase):
        out = []
        for d in range(2):
            out.append((remote(xs.at[phase, d], xr.at[phase, 1 - d], phase, 2 + 1 - d, moved(d, None, None)), there[0][d]))
            out.append((remote(ys.at[phase, d], yr.at[phase, 1 - d], phase, 4 + 1 - d, moved(None, d, None)), there[1][d]))
            for e in range(2):
                slot = 6 + 2 * (1 - d) + 1 - e
                out.append((remote(es.at[phase, 2 * d + e], er.at[phase, 2 * (1 - d) + 1 - e], phase, slot,
                                   moved(d, e, None)), there[0][d] & there[1][e]))
        return out

    def each(copies, act, flip):
        n = len(copies)
        for index, (copy, exists) in enumerate(copies):
            @pl.when(exists)
            def _():
                act(copy)

    def send_z(phase):
        packed = None
        for t in range(nt):
            part = jnp.where(face_c, field[:, tile(t)], 0.0)
            part = part if t == 0 else pltpu.roll(part, 2 * t, 1)
            packed = part if packed is None else packed + part
        zs[phase] = packed
        for copy, exists in z_copies(phase):
            @pl.when(exists)
            def _():
                copy.start()

    def wait_slot(ref, slot_sem):
        pltpu.make_async_copy(ref, ref, slot_sem).wait()

    def finish_halo(phase):
        for d in range(2):
            @pl.when(there[2][d])
            def _():
                wait_slot(zr.at[phase, d], hrecv.at[phase, d])
        merged = jnp.where(even, pltpu.roll(zr[phase, 0], LANES - last, 1), pltpu.roll(zr[phase, 1], last, 1))
        for t in range(nt):
            part = merged if t == 0 else pltpu.roll(merged, LANES - 2 * t, 1)
            field[:, tile(t)] += jnp.where(face_c, part, 0.0)
        for d in range(2):
            row = 0 if d == 0 else last
            for t in range(nt):
                xs[phase, d, t:t + 1, :] = field[row:row + 1, tile(t)]
            for e in range(2):
                es[phase, 2 * d + e] = field[row:row + 1, tile(0 if e == 0 else nt - 1)]
            packed = None
            for i in range(ni):
                block = field[SUB * i:SUB * (i + 1), tile(0 if d == 0 else nt - 1)]
                part = jnp.where(low8 if d == 0 else high8, block, 0.0)
                shift = (count * i + d * count) % LANES
                part = part if shift == 0 else pltpu.roll(part, shift, 1)
                packed = part if packed is None else packed + part
            ys[phase, d] = packed
        for copy, exists in xy_copies(phase):
            @pl.when(exists)
            def _():
                copy.start()

    def add_halo(phase):
        for d in range(2):
            @pl.when(there[0][d])
            def _():
                wait_slot(xr.at[phase, d], hrecv.at[phase, 2 + d])

            @pl.when(there[1][d])
            def _():
                wait_slot(yr.at[phase, d], hrecv.at[phase, 4 + d])
            for e in range(2):
                @pl.when(there[0][d] & there[1][e])
                def _():
                    wait_slot(er.at[phase, 2 * d + e], hrecv.at[phase, 6 + 2 * d + e])
        for d in range(2):
            received = yr[phase, d]
            for i in range(ni):
                shift = (-count * i - d * count) % LANES
                part = received if shift == 0 else pltpu.roll(received, shift, 1)
                field[SUB * i:SUB * (i + 1), tile(0 if d == 0 else nt - 1)] += jnp.where(low8 if d == 0 else high8, part, 0.0)
        for d in range(2):
            row = 0 if d == 0 else last
            for t in range(nt):
                line = xr[phase, d, t:t + 1, :]
                if t == 0:
                    line += jnp.where(lane1 < count, pltpu.roll(er[phase, 2 * d], count, 1), 0.0)
                if t == nt - 1:
                    line += jnp.where(lane1 >= LANES - count, pltpu.roll(er[phase, 2 * d + 1], LANES - count, 1), 0.0)
                field[row:row + 1, tile(t)] += line

    def send_dots(phase, products):
        packed = None
        for k, product in enumerate(products):
            acc = None
            for i in range(ni):
                for t in range(nt):
                    block = product[SUB * i:SUB * (i + 1), tile(t)]
                    acc = block if acc is None else acc + block
            line = jnp.where(iota((SUB, LANES), 0) == k, jnp.sum(acc, axis=0, keepdims=True), 0.0)
            packed = line if packed is None else packed + line
        sums = jnp.sum(packed, axis=1, keepdims=True)
        rows[phase, me] = jnp.sum(jnp.where(diag, sums, 0.0), axis=0, keepdims=True)

        def send(k, carry):
            pltpu.make_async_remote_copy(
                src_ref=rows.at[phase, me], dst_ref=rows.at[phase, me], send_sem=rsend.at[phase],
                recv_sem=rrecv.at[phase], device_id=peer(k), device_id_type=MESH).start()
            return carry

        lax.fori_loop(1, total, send, 0)

    def take_dots(phase):
        others = rows.at[phase, pl.ds(0, total - 1)]
        pltpu.make_async_copy(others, others, rrecv.at[phase]).wait()
        line = jnp.sum(rows[phase], axis=0)
        return jnp.sum(jnp.where(diag, line, 0.0), axis=1, keepdims=True)

    build_matrices(st, mx, my, mz)
    pl.semaphore_wait(barrier, total - 1)
    send_z(0)
    finish_halo(0)
    add_halo(0)
    vector = field[...]
    alpha = None
    row2, col2 = iota(coef.shape[1:], 0), iota(coef.shape[1:], 1)
    coefs = jnp.zeros(coef.shape[1:], F32)
    for j in range(ITERS):
        phase = j + 1
        image = apply_patch(vector, mx[...], my[...], mz[...])
        field[...] = image
        send_z(phase)
        old = [v0[...] if i == 0 else basis[i - 1] for i in range(j)]
        send_dots(phase, [wt[...] * vector * vector, image * vector] + [image * v for v in old])
        finish_halo(phase)
        add_halo(phase)
        sums = take_dots(phase)
        norm = jnp.sqrt(sums[0:1])
        inverse = 1.0 / norm
        if j > 0:
            coefs = jnp.where((row2 == 1) & (col2 == j - 1), norm * alpha, coefs)
        alpha = sums[1:2] / sums[0:1]
        coefs = jnp.where((row2 == 0) & (col2 == j), alpha, coefs)
        unit = vector * inverse
        if j == 0:
            v0[...] = unit
        else:
            basis[j - 1] = unit
        factor = inverse / alpha
        following = field[...] * factor - unit
        for i in range(j):
            following = following - (sums[2 + i:3 + i] * factor) * old[i]
        vector = following
    send_dots(ITERS + 1, [wt[...] * vector * vector])
    sums = take_dots(ITERS + 1)
    norm = jnp.sqrt(sums[0:1])
    coefs = jnp.where((row2 == 1) & (col2 == ITERS - 1), norm * alpha, coefs)
    basis[ITERS - 1] = vector * (1.0 / norm)
    coef[0] = coefs

    for phase in range(ITERS + 1):
        for copy, exists in z_copies(phase) + xy_copies(phase):
            @pl.when(exists)
            def _():
                copy.wait_send()
    for phase in range(1, ITERS + 2):
        others = rows.at[phase, pl.ds(0, total - 1)]
        pltpu.make_async_copy(others, others, rsend.at[phase]).wait()


def shards(sizes, start, stencils):
    probes, count, area = start.shape[3:]
    nt = area // LANES
    total = sizes[0] * sizes[1] * sizes[2]
    halos = ITERS + 1
    vmem = pl.BlockSpec(memory_space=pltpu.VMEM)
    call = pl.pallas_call(
        functools.partial(kernel, sizes),
        out_shape=(jax.ShapeDtypeStruct((ITERS, count, area), F32), jax.ShapeDtypeStruct((1, 2, ITERS), F32)),
        in_specs=[vmem, vmem],
        out_specs=(vmem, vmem),
        scratch_shapes=[
            pltpu.VMEM((count, 6 * count), BF16),
            pltpu.VMEM((4 * count, 6 * count), BF16),
            pltpu.VMEM((3 * LANES, 2 * LANES), BF16),
            pltpu.VMEM((count, area), F32),
            pltpu.VMEM((count, area), F32),
            pltpu.VMEM((count, area), F32),
            pltpu.VMEM((halos, count, LANES), F32),
            pltpu.VMEM((halos, 2, count, LANES), F32),
            pltpu.VMEM((halos, 2, nt, LANES), F32),
            pltpu.VMEM((halos, 2, nt, LANES), F32),
            pltpu.VMEM((halos, 2, SUB, LANES), F32),
            pltpu.VMEM((halos, 2, SUB, LANES), F32),
            pltpu.VMEM((halos, 4, 1, LANES), F32),
            pltpu.VMEM((halos, 4, 1, LANES), F32),
            pltpu.VMEM((halos + 1, total, 1, LANES), F32),
            pltpu.SemaphoreType.DMA((halos, 10)),
            pltpu.SemaphoreType.DMA((halos, 10)),
            pltpu.SemaphoreType.DMA((halos + 1,)),
            pltpu.SemaphoreType.DMA((halos + 1,)),
        ],
        compiler_params=pltpu.CompilerParams(collective_id=0, has_side_effects=True, vmem_limit_bytes=48 * 1024 * 1024),
    )
    results = [call(start[0, 0, 0, p], stencils[:, 0, 0, 0]) for p in range(probes)]
    basis = jnp.stack([r[0] for r in results])
    return basis[None, None, None], jnp.concatenate([r[1] for r in results])


def solution(mesh):
    sizes = tuple(mesh.shape[name] for name in ("gx", "gy", "gz"))
    return jax.shard_map(
        functools.partial(shards, sizes),
        mesh=mesh,
        in_specs=(P("gx", "gy", "gz", None, None, None), P(None, "gx", "gy", "gz", None, None)),
        out_specs=(P("gx", "gy", "gz", None, None, None, None), P()),
        check_vma=False,
    )
```

```python
import functools

import jax
import jax.numpy as jnp
from jax import lax
from jax.experimental import pallas as pl
from jax.experimental.pallas import tpu as pltpu
from jax.sharding import PartitionSpec as P

ITERS = 5
LANES = 128
SUB = 8
MESH = pl.DeviceIdType.MESH
F32 = jnp.float32
BF16 = jnp.bfloat16
HIGHEST = lax.Precision.HIGHEST


def iota(shape, dim):
    return lax.broadcasted_iota(jnp.int32, shape, dim)


def split(x):
    hi = x.astype(BF16)
    return hi, (x - hi.astype(F32)).astype(BF16)


def exact(a, b):
    return lax.dot_general(a, b, (((1,), (0,)), ((), ())), precision=HIGHEST, preferred_element_type=F32)


def mul(a, b):
    return jnp.dot(a, b, preferred_element_type=F32)


def swap(x):
    sub = iota((1, SUB, LANES), 1)
    group = iota((1, SUB, LANES), 2) >> 5
    s0, s1 = sub & 1, (sub >> 1) & 1
    g0, g1 = group & 1, (group >> 1) & 1
    far = pltpu.roll(x, 64, 2)
    x = jnp.where(s1 == g1, x, jnp.where(s1 == 0, pltpu.roll(far, SUB - 2, 1), pltpu.roll(far, 2, 1)))
    up = pltpu.roll(pltpu.roll(x, SUB - 1, 1), 32, 2)
    down = pltpu.roll(pltpu.roll(x, 1, 1), LANES - 32, 2)
    return jnp.where(s0 == g0, x, jnp.where(s0 == 0, up, down))


def build_matrices(st, mx, my, mz):
    count = st.shape[1]
    wide = LANES
    spread = ((iota((wide, count), 0) & (count - 1)) == iota((wide, count), 1)).astype(F32)
    spread_t = ((iota((count, wide), 1) & (count - 1)) == iota((count, wide), 0)).astype(F32)
    same = (iota((wide, wide), 0) >> 5) == (iota((wide, wide), 1) >> 5)
    for slot, which in ((0, 5), (1, 2)):
        big = exact(exact(spread, st[which].T), spread_t)
        hi, lo = split(jnp.where(same, big, 0.0))
        mz[0:wide, slot * wide:(slot + 1) * wide] = hi
        mz[wide:2 * wide, slot * wide:(slot + 1) * wide] = hi
        mz[2 * wide:3 * wide, slot * wide:(slot + 1) * wide] = lo
    rows = 2 * count
    r = iota((rows, count), 0)
    pick = (((r >> 3) * 4 + (r & 3)) == iota((rows, count), 1)).astype(F32)
    cols = 3 * rows
    l = iota((count, cols), 1) & (rows - 1)
    pick_t = (((l >> 3) * 4 + (l & 3)) == iota((count, cols), 0)).astype(F32)
    same = ((iota((rows, cols), 0) >> 2) & 1) == ((iota((rows, cols), 1) >> 2) & 1)
    middle = (iota((rows, cols), 1) >= rows) & (iota((rows, cols), 1) < 2 * rows)
    for slot, which in ((0, 4), (1, 1)):
        big = jnp.where(same, exact(exact(pick, st[which]), pick_t), 0.0)
        hi = big.astype(BF16).astype(F32)
        my[slot * rows:(slot + 1) * rows, :] = jnp.where(middle, big - hi, hi).astype(BF16)
    cols = 6 * count
    tile = ((iota((count, cols), 1) & (count - 1)) == iota((count, cols), 0)).astype(F32)
    stiff = exact(st[0], tile)
    mass = exact(st[3], tile)
    block = iota((count, cols), 1) >> 5
    big = jnp.where(block < 3, stiff, mass)
    hi = big.astype(BF16).astype(F32)
    mx[...] = jnp.where((block == 1) | (block == 4), big - hi, hi).astype(BF16)


def apply_patch(u, mx, my, mz):
    count, area = u.shape
    ni, nt = count // SUB, area // LANES
    tiles = jnp.concatenate(
        [u[SUB * i:SUB * (i + 1), LANES * t:LANES * (t + 1)] for i in range(ni) for t in range(nt)], axis=0
    )
    tiles = swap(tiles.reshape(ni * nt, SUB, LANES)).reshape(ni * nt * SUB, LANES)
    hi, lo = split(tiles)
    z = mul(jnp.concatenate([hi, lo, hi], axis=1), mz)
    rows = nt * SUB
    packed = []
    for slot in range(2):
        part = z[:, slot * LANES:(slot + 1) * LANES]
        wide = jnp.concatenate([part[rows * i:rows * (i + 1)] for i in range(ni)], axis=1)
        hi, lo = split(wide)
        packed.append(jnp.concatenate([hi, hi, lo], axis=0))
    both = mul(my, packed[0])
    first = both[:rows]
    second = both[rows:] + mul(my[:rows], packed[1])
    pieces = []
    for term in (first, second):
        stacked = jnp.concatenate([term[:, LANES * i:LANES * (i + 1)] for i in range(ni)], axis=0)
        stacked = swap(stacked.reshape(ni * nt, SUB, LANES))
        back = jnp.concatenate(
            [jnp.concatenate([stacked[i * nt + t] for i in range(ni)], axis=0) for t in range(nt)], axis=1
        )
        hi, lo = split(back)
        pieces += [hi, hi, lo]
    return mul(mx, jnp.concatenate(pieces, axis=0))


def kernel(sizes, start, st, basis, coef, mx, my, mz, wt, v0, field,
           zs, zr, xs, xr, ys, yr, es, er, rows, hsend, hrecv, rsend, rrecv, ready, locals_, images):
    nx, ny, nz = sizes
    total = nx * ny * nz
    count, area = start.shape
    nt = area // LANES
    ni = count // SUB
    last = count - 1
    px, py, pz = lax.axis_index("gx"), lax.axis_index("gy"), lax.axis_index("gz")
    me = (px * ny + py) * nz + pz
    coords = (px, py, pz)
    there = [[coords[d] > 0, coords[d] < sizes[d] - 1] for d in range(3)]

    for ref in (zr, xr, yr, er):
        ref[...] = jnp.zeros_like(ref)
    barrier = pltpu.get_barrier_semaphore()

    def peer(k):
        p = lax.rem(me + k, total)
        return (p // (ny * nz), (p // nz) % ny, p % nz)

    def every_peer(act):
        if total > 64:
            def step(k, carry):
                act(peer(k))
                return carry

            lax.fori_loop(1, total, step, 0)
            return
        around = [[lax.rem(coords[d] + k, sizes[d]) if k else coords[d] for k in range(sizes[d])] for d in range(3)]
        for ky in range(ny - 1, -1, -1):
            for kx in range(nx - 1, -1, -1):
                for kz in range(nz):
                    if kx or ky or kz:
                        act((around[0][kx], around[1][ky], around[2][kz]))

    def neighbours(act):
        for dx in (-1, 0, 1):
            for dy in (-1, 0, 1):
                for dz in (-1, 0, 1):
                    if dx or dy or dz:
                        target = (px + dx, py + dy, pz + dz)
                        inside = None
                        for d, step in enumerate((dx, dy, dz)):
                            if step:
                                side = there[d][(step + 1) // 2]
                                inside = side if inside is None else inside & side

                        @pl.when(inside)
                        def _():
                            act(target)

    around_me = 1
    for d in range(3):
        around_me = around_me * (1 + (coords[d] > 0).astype(jnp.int32) + (coords[d] < sizes[d] - 1).astype(jnp.int32))
    around_me = around_me - 1

    rounds = max(sizes) - 2

    def call(r):
        neighbours(lambda target: pl.semaphore_signal(ready.at[r], inc=1, device_id=target, device_id_type=MESH))

    neighbours(lambda target: pl.semaphore_signal(barrier, inc=1, device_id=target, device_id_type=MESH))

    def shared(index, d):
        return ((index == 0) & there[d][0]) | ((index == last) & there[d][1])

    lane = iota((count, area), 1)
    ia, ib, ic = iota((count, area), 0), lane >> 5, lane & (count - 1)
    half = lambda index, d: jnp.where(shared(index, d), 0.5, 1.0)
    weight = half(ia, 0) * half(ib, 1) * half(ic, 2)
    wt[...] = weight.astype(F32)
    field[...] = start[...] * wt[...]

    lane_c = iota((count, LANES), 1)
    face_c = (lane_c & (count - 1) == 0) | (lane_c & (count - 1) == last)
    even = (lane_c & 1) == 0
    lane8 = iota((SUB, LANES), 1)
    low8, high8 = lane8 < count, lane8 >= LANES - count
    lane1 = iota((1, LANES), 1)
    diag = iota((SUB, LANES), 0) == lane8

    def tile(t):
        return slice(t * LANES, (t + 1) * LANES)

    def halo_copies(phase):
        out = []

        def add(src, dst, slot, *direction):
            there_all, target = None, {}
            for d, step in enumerate(direction):
                if step is not None:
                    there_all = there[d][step] if there_all is None else there_all & there[d][step]
            target = tuple(c if step is None else c + 2 * step - 1 for c, step in zip(coords, direction))
            copy = pltpu.make_async_remote_copy(
                src_ref=src, dst_ref=dst.at[phase, slot], send_sem=hsend.at[phase, len(out)],
                recv_sem=hrecv.at[phase, len(out)], device_id=target, device_id_type=MESH)
            out.append((copy, there_all, direction, dst, slot))

        for z in (1, 0, None):
            for d in range(2):
                for e in range(2):
                    back = 0 if z is None else 2 - z
                    add(es.at[phase, 2 * d + e], er, (2 * (1 - d) + 1 - e) * 3 + back, d, e, z)
        for z in (1, 0, None):
            back = 0 if z is None else 2 - z
            for d in range(2):
                add(xs.at[phase, d], xr, (1 - d) * 3 + back, d, None, z)
        for z in (1, 0, None):
            back = 0 if z is None else 2 - z
            for d in range(2):
                add(ys.at[phase, d], yr, (1 - d) * 3 + back, None, d, z)
        for d in range(2):
            add(zs.at[phase], zr, 1 - d, None, None, d)
        return out

    def start_all(copies):
        for copy, exists, *_ in copies:
            @pl.when(exists)
            def _():
                copy.start()

    def send_halo(phase):
        copies = halo_copies(phase)
        for d in range(2):
            row = 0 if d == 0 else last
            for e in range(2):
                es[phase, 2 * d + e] = field[row:row + 1, tile(0 if e == 0 else nt - 1)]
            for t in range(nt):
                xs[phase, d, t:t + 1, :] = field[row:row + 1, tile(t)]
            packed = None
            for i in range(ni):
                block = field[SUB * i:SUB * (i + 1), tile(0 if d == 0 else nt - 1)]
                part = jnp.where(low8 if d == 0 else high8, block, 0.0)
                shift = (count * i + d * count) % LANES
                part = part if shift == 0 else pltpu.roll(part, shift, 1)
                packed = part if packed is None else packed + part
            ys[phase, d] = packed
        packed = None
        for t in range(nt):
            part = jnp.where(face_c, field[:, tile(t)], 0.0)
            part = part if t == 0 else pltpu.roll(part, 2 * t, 1)
            packed = part if packed is None else packed + part
        zs[phase] = packed
        start_all(copies)

    def fold(ref, phase, base):
        low = ref[phase, base + 1]
        c = iota(low.shape, 1) & (count - 1)
        out = ref[phase, base] + jnp.where(c == 0, pltpu.roll(low, LANES - last, 1), 0.0)
        return out + jnp.where(c == last, pltpu.roll(ref[phase, base + 2], last, 1), 0.0)

    def add_halo(phase):
        copies = halo_copies(phase)
        for index, (copy, _, direction, dst, slot) in enumerate(copies):
            mirror = None
            for d, step in enumerate(direction):
                if step is not None:
                    mirror = there[d][1 - step] if mirror is None else mirror & there[d][1 - step]

            @pl.when(mirror)
            def _():
                into = dst.at[phase, slot]
                pltpu.make_async_copy(into, into, hrecv.at[phase, index]).wait()
        merged = jnp.where(even, pltpu.roll(zr[phase, 0], LANES - last, 1), pltpu.roll(zr[phase, 1], last, 1))
        for t in range(nt):
            part = merged if t == 0 else pltpu.roll(merged, LANES - 2 * t, 1)
            field[:, tile(t)] += jnp.where(face_c, part, 0.0)
        for d in range(2):
            received = fold(yr, phase, 3 * d)
            for i in range(ni):
                shift = (-count * i - d * count) % LANES
                part = received if shift == 0 else pltpu.roll(received, shift, 1)
                field[SUB * i:SUB * (i + 1), tile(0 if d == 0 else nt - 1)] += jnp.where(low8 if d == 0 else high8, part, 0.0)
        for d in range(2):
            row = 0 if d == 0 else last
            received = fold(xr, phase, 3 * d)
            for t in range(nt):
                line = received[t:t + 1]
                if t == 0:
                    line += jnp.where(lane1 < count, pltpu.roll(fold(er, phase, 6 * d), count, 1), 0.0)
                if t == nt - 1:
                    line += jnp.where(lane1 >= LANES - count, pltpu.roll(fold(er, phase, 6 * d + 3), LANES - count, 1), 0.0)
                field[row:row + 1, tile(t)] += line

    def send_dots(phase, products):
        packed = None
        for k, product in enumerate(products):
            acc = None
            for i in range(ni):
                for t in range(nt):
                    block = product[SUB * i:SUB * (i + 1), tile(t)]
                    acc = block if acc is None else acc + block
            line = jnp.where(iota((SUB, LANES), 0) == k, jnp.sum(acc, axis=0, keepdims=True), 0.0)
            packed = line if packed is None else packed + line
        sums = jnp.sum(packed, axis=1, keepdims=True)
        rows[phase, me] = jnp.sum(jnp.where(diag, sums, 0.0), axis=0, keepdims=True)

        def send(target):
            pltpu.make_async_remote_copy(
                src_ref=rows.at[phase, me], dst_ref=rows.at[phase, me], send_sem=rsend.at[phase],
                recv_sem=rrecv.at[phase], device_id=target, device_id_type=MESH).start()

        every_peer(send)

    def take_dots(phase):
        others = rows.at[phase, pl.ds(0, total - 1)]
        pltpu.make_async_copy(others, others, rrecv.at[phase]).wait()
        line = jnp.sum(rows[phase], axis=0)
        return jnp.sum(jnp.where(diag, line, 0.0), axis=1, keepdims=True)

    build_matrices(st, mx, my, mz)
    pl.semaphore_wait(barrier, around_me)
    send_halo(0)
    for r in range(rounds):
        call(r)
        if r < rounds - 1:
            pl.semaphore_wait(ready.at[r], around_me)
    add_halo(0)
    vector = field[...]
    alpha = None
    row2, col2 = iota(coef.shape[1:], 0), iota(coef.shape[1:], 1)
    coefs = jnp.zeros(coef.shape[1:], F32)
    local = apply_patch(vector, mx[...], my[...], mz[...])
    field[...] = local
    send_halo(1)
    if rounds > 0:
        pl.semaphore_wait(ready.at[rounds - 1], around_me)
    send_dots(1, [wt[...] * vector * vector, local * vector])
    add_halo(1)
    image = field[...]
    for j in range(ITERS):
        more = j < ITERS - 1
        if more:
            ahead = apply_patch(image, mx[...], my[...], mz[...])
            field[...] = ahead
            send_halo(j + 2)
        sums = take_dots(j + 1)
        norm = jnp.sqrt(sums[0:1])
        inverse = 1.0 / norm
        if j > 0:
            coefs = jnp.where((row2 == 1) & (col2 == j - 1), norm * alpha, coefs)
        alpha = sums[1:2] / sums[0:1]
        coefs = jnp.where((row2 == 0) & (col2 == j), alpha, coefs)
        factor = inverse / alpha
        heights = [sums[2 + i:3 + i] * factor for i in range(j)]

        def follow(applied, unit, old):
            out = applied * factor - unit
            for i in range(j):
                out = out - heights[i] * old(i)
            return out

        old_vector = lambda i: v0[...] if i == 0 else basis[i - 1]
        unit = vector * inverse
        if j == 0:
            v0[...] = unit
        else:
            basis[j - 1] = unit
        vector = follow(image, unit, old_vector)
        if more:
            unit = local * inverse
            locals_[j] = unit
            local = follow(ahead, unit, lambda i: locals_[i])
            send_dots(j + 2, [wt[...] * vector * vector, local * vector] + [local * old_vector(i) for i in range(j + 1)])
            unit = image * inverse
            images[j] = unit
            add_halo(j + 2)
            image = follow(field[...], unit, lambda i: images[i])
    send_dots(ITERS + 1, [wt[...] * vector * vector])
    sums = take_dots(ITERS + 1)
    norm = jnp.sqrt(sums[0:1])
    coefs = jnp.where((row2 == 1) & (col2 == ITERS - 1), norm * alpha, coefs)
    basis[ITERS - 1] = vector * (1.0 / norm)
    coef[0] = coefs

    for phase in range(ITERS + 1):
        for copy, exists, *_ in halo_copies(phase):
            @pl.when(exists)
            def _():
                copy.wait_send()
    for phase in range(1, ITERS + 2):
        others = rows.at[phase, pl.ds(0, total - 1)]
        pltpu.make_async_copy(others, others, rsend.at[phase]).wait()


def shards(sizes, start, stencils):
    probes, count, area = start.shape[3:]
    nt = area // LANES
    total = sizes[0] * sizes[1] * sizes[2]
    halos = ITERS + 1
    vmem = pl.BlockSpec(memory_space=pltpu.VMEM)
    call = pl.pallas_call(
        functools.partial(kernel, sizes),
        out_shape=(jax.ShapeDtypeStruct((ITERS, count, area), F32), jax.ShapeDtypeStruct((1, 2, ITERS), F32)),
        in_specs=[vmem, vmem],
        out_specs=(vmem, vmem),
        scratch_shapes=[
            pltpu.VMEM((count, 6 * count), BF16),
            pltpu.VMEM((4 * count, 6 * count), BF16),
            pltpu.VMEM((3 * LANES, 2 * LANES), BF16),
            pltpu.VMEM((count, area), F32),
            pltpu.VMEM((count, area), F32),
            pltpu.VMEM((count, area), F32),
            pltpu.VMEM((halos, count, LANES), F32),
            pltpu.VMEM((halos, 2, count, LANES), F32),
            pltpu.VMEM((halos, 2, nt, LANES), F32),
            pltpu.VMEM((halos, 6, nt, LANES), F32),
            pltpu.VMEM((halos, 2, SUB, LANES), F32),
            pltpu.VMEM((halos, 6, SUB, LANES), F32),
            pltpu.VMEM((halos, 4, 1, LANES), F32),
            pltpu.VMEM((halos, 12, 1, LANES), F32),
            pltpu.VMEM((halos + 1, total, 1, LANES), F32),
            pltpu.SemaphoreType.DMA((halos, 26)),
            pltpu.SemaphoreType.DMA((halos, 26)),
            pltpu.SemaphoreType.DMA((halos + 1,)),
            pltpu.SemaphoreType.DMA((halos + 1,)),
            pltpu.SemaphoreType.REGULAR((max(1, max(sizes) - 2),)),
            pltpu.VMEM((ITERS - 1, count, area), F32),
            pltpu.VMEM((ITERS - 1, count, area), F32),
        ],
        compiler_params=pltpu.CompilerParams(collective_id=0, has_side_effects=True, vmem_limit_bytes=48 * 1024 * 1024),
    )
    results = [call(start[0, 0, 0, p], stencils[:, 0, 0, 0]) for p in range(probes)]
    basis = jnp.stack([r[0] for r in results])
    return basis[None, None, None], jnp.concatenate([r[1] for r in results])


def solution(mesh):
    sizes = tuple(mesh.shape[name] for name in ("gx", "gy", "gz"))
    return jax.shard_map(
        functools.partial(shards, sizes),
        mesh=mesh,
        in_specs=(P("gx", "gy", "gz", None, None, None), P(None, "gx", "gy", "gz", None, None)),
        out_specs=(P("gx", "gy", "gz", None, None, None, None), P()),
        check_vma=False,
    )
```
